32 devices in a mesh: dp: 4 (over z), mp: 8 (over y, x, core).
Axes of the slice: x: 2, y: 2, z: 4, core: 2. Of those that a mesh axis runs over, the one named last changes fastest.
Arguments:
- weight: bfloat16 [5120, 32768], P('dp', 'mp'), may hold values from -0.078125 to 0.078125
- rank_map: int32 [8], replicated, may hold values from 0 to 7, each once
Outputs:
- quant_out: bfloat16 [5120, 32768], P(None, 'mp')
- scale_out: bfloat16 [5120, 256], P(None, 'mp')
- checksum: float32 [256], replicated
The draws below stay inside these ranges and needn't reach their ends.
Inputs may be any that keep to these rules, and one draw needn't show every extreme that they name: `rank_map`: a permutation of 0 to 7.
All inputs are finite; a program needn't handle non-finite values.
Results may differ from the reference program's by a relative error of at most 0.0085.
Values may be sent and summed in bfloat16 or wider, within the bound.
No kernel may reach another device: no remote copies, remote signals or barrier semaphores. Data moves between devices by JAX's collectives and lax.ppermute only.
A program may use at most 192 MiB of HBM per device.

```python
import math
import jax
import jax.numpy as jnp
from jax import lax

D = 5120
F = 32768
N_MP = 8


def level_of(key, shape, pieces, smallest, largest):
    factor_of = 1.0
    for position, parts in pieces:
        draws = jax.random.uniform(jax.random.fold_in(jax.random.fold_in(key, 6), position), (parts,), jnp.float32, smallest / len(pieces), largest / len(pieces))
        factor_of = factor_of * jnp.repeat(jnp.exp(draws), shape[position] // parts).reshape((-1,) + (1,) * (len(shape) - 1 - position))
    return factor_of


def scatter_about(stream_key, dims, deviation, limit, shards=(), dtype=jnp.bfloat16):
    values = jax.random.normal(stream_key, dims, jnp.float32) * deviation
    if len(shards) > 0:
        values = level_of(stream_key, dims, shards, -0.22, 0.18) * values
    return jnp.clip(values, min=-limit, max=limit).astype(dtype)


def setup_inputs(seed: int = 0) -> dict:
    key_of = jax.random.split(jax.random.key(seed), 3)
    weight = scatter_about(key_of[0], (D, F), D ** -0.5, 0.078125, ((0, 4), (1, 8)))
    rank_map = jax.random.permutation(key_of[1], N_MP).astype(jnp.int32)
    return {"weight": weight, "rank_map": rank_map}


floor_ratio = 0.25

def quantize(weight):
    rows, cols = weight.shape
    blocks = weight.astype(jnp.float32).reshape(rows, cols // 128, 128)
    peak = lax.optimization_barrier(jnp.max(jnp.abs(blocks), axis=2))
    scale = (jnp.maximum(peak, floor_ratio / math.sqrt(D)) / 127.0).astype(jnp.bfloat16)
    quant = (blocks / scale.astype(jnp.float32)[:, :, None]).astype(jnp.bfloat16)
    return (quant, scale)

def inverse(rank_map):
    count = rank_map.shape[0]
    ids = jnp.arange(count).astype(jnp.int32)
    match = (rank_map[None, :] == ids[:, None]).astype(jnp.int32)
    return lax.optimization_barrier(jnp.sum(ids[None, :] * match, axis=1)).astype(jnp.int32)

def reference(weight, rank_map):
    quant, scale = quantize(weight)
    total = lax.optimization_barrier(jnp.sum(quant.astype(jnp.float32), axis=(0, 2)))
    checksum = total / (127.0 * math.sqrt(D * 128))
    inv = inverse(rank_map)
    blocks = F // 128
    local = blocks // N_MP
    order = (jnp.arange(local).astype(jnp.int32)[None, :] * N_MP + inv[:, None]).reshape(-1).astype(jnp.int32)
    quant_out = jnp.take(quant, order, axis=1).reshape(D, F)
    scale_out = jnp.take(scale, order, axis=1)
    return (quant_out, scale_out, checksum)
```

```python
import functools
import math

import jax
import jax.numpy as jnp
from jax import lax
from jax.experimental import pallas as pl
from jax.experimental.pallas import tpu as pltpu
from jax.sharding import PartitionSpec as P

D = 5120
LANES = 128
UNITS = 20
CHUNKS = (2, 3, 5, 5, 5)


floor_ratio = 0.25


def block_scale(values):
    peak = jnp.max(jnp.abs(values), axis=1, keepdims=True)
    return (jnp.maximum(peak, floor_ratio / math.sqrt(D)) / 127.0).astype(jnp.bfloat16)


def block_quant(values, scale):
    return (values * (1.0 / scale.astype(jnp.float32))).astype(jnp.bfloat16)


def inverse(rank_map):
    count = rank_map.shape[0]
    ids = jnp.arange(count, dtype=jnp.int32)
    match = (rank_map[None, :] == ids[:, None]).astype(jnp.int32)
    return jnp.sum(ids[None, :] * match, axis=1)


def pack_kernel(inv_ref, w_ref, out_ref):
    count, _, width = out_ref.shape
    for dest in range(count):
        for i in range(width // LANES):
            start = pl.multiple_of((i * count + inv_ref[dest]) * LANES, LANES)
            out_ref[dest, :, i * LANES : (i + 1) * LANES] = w_ref[:, pl.ds(start, LANES)]


def pack(weight, inv, first, rows, tile):
    count = inv.shape[0]
    cols = weight.shape[1]
    width = cols // count
    return pl.pallas_call(
        pack_kernel,
        grid_spec=pltpu.PrefetchScalarGridSpec(
            num_scalar_prefetch=1,
            grid=(rows // tile,),
            in_specs=[pl.BlockSpec((tile, cols), lambda g, inv: (g + first // tile, 0))],
            out_specs=pl.BlockSpec((count, tile, width), lambda g, inv: (0, g, 0)),
        ),
        out_shape=jax.ShapeDtypeStruct((count, rows, width), weight.dtype),
        cost_estimate=pl.CostEstimate(flops=rows * cols, bytes_accessed=4 * rows * cols, transcendentals=0),
        name="pack",
    )(inv, weight)


def place_tile(piece_ref, quant_ref, scale_ref):
    count, tile, width = piece_ref.shape
    per = width // LANES
    lane = lax.broadcasted_iota(jnp.int32, (tile, LANES), 1)
    scales = jnp.zeros((tile, LANES), jnp.float32)
    for source in range(count):
        for i in range(per):
            block = source * per + i
            values = piece_ref[source, :, i * LANES : (i + 1) * LANES].astype(jnp.float32)
            scale = block_scale(values)
            quant_ref[:, block * LANES : (block + 1) * LANES] = block_quant(values, scale)
            scales = jnp.where(lane == block, scale.astype(jnp.float32), scales)
    scale_ref[...] = scales[:, : count * per].astype(jnp.bfloat16)


def place_kernel(tile, at_ref, piece_ref, *refs):
    quant_ref, scale_ref = refs[-2:]
    count, rows, width = piece_ref.shape
    nblocks = scale_ref.shape[1]

    @pl.when(at_ref[1] == 1)
    def _():
        base = at_ref[0]
        pltpu.emit_pipeline(
            place_tile,
            grid=(rows // tile,),
            in_specs=[pl.BlockSpec((count, tile, width), lambda g: (0, g, 0))],
            out_specs=[
                pl.BlockSpec((tile, count * width), lambda g: (base + g, 0)),
                pl.BlockSpec((tile, nblocks), lambda g: (base + g, 0)),
            ],
        )(piece_ref, quant_ref, scale_ref)


def place(outs, piece, row, valid, total, tile):
    count, rows, width = piece.shape
    at = jnp.stack([row // tile, valid.astype(jnp.int32)])
    whole = pl.BlockSpec(memory_space=pl.ANY)
    held = () if outs is None else outs
    return pl.pallas_call(
        functools.partial(place_kernel, tile),
        in_specs=[pl.BlockSpec(memory_space=pltpu.SMEM)] + [whole] * (1 + len(held)),
        out_specs=[whole, whole],
        out_shape=[
            jax.ShapeDtypeStruct((total, count * width), jnp.bfloat16),
            jax.ShapeDtypeStruct((total, count * width // LANES), jnp.bfloat16),
        ],
        input_output_aliases={2: 0, 3: 1} if held else {},
        cost_estimate=pl.CostEstimate(
            flops=8 * piece.size, bytes_accessed=4 * piece.size, transcendentals=0
        ),
        name="place",
    )(at, piece, *held)


def sums_kernel(w_ref, out_ref):
    tile, cols = w_ref.shape

    @pl.when(pl.program_id(0) == 0)
    def _():
        out_ref[...] = jnp.zeros_like(out_ref)

    for block in range(cols // LANES):
        span = slice(block * LANES, (block + 1) * LANES)
        values = w_ref[:, span].astype(jnp.float32)
        quant = block_quant(values, block_scale(values)).astype(jnp.float32)
        out_ref[:, span] += jnp.sum(quant.reshape(tile // 8, 8, LANES), axis=0)


def column_sums(weight, tile):
    rows, cols = weight.shape
    return pl.pallas_call(
        sums_kernel,
        grid=(rows // tile,),
        in_specs=[pl.BlockSpec((tile, cols), lambda g: (g, 0))],
        out_specs=pl.BlockSpec((8, cols), lambda g: (0, 0)),
        out_shape=jax.ShapeDtypeStruct((8, cols), jnp.float32),
        cost_estimate=pl.CostEstimate(flops=8 * rows * cols, bytes_accessed=2 * rows * cols, transcendentals=0),
        name="sums",
    )(weight)


def local(weight, rank_map):
    count = lax.axis_size("mp")
    rank = lax.axis_index("mp")
    depth = lax.axis_size("dp")
    level = lax.axis_index("dp")
    rows, cols = weight.shape
    tile = rows // UNITS
    total = rows * depth
    inv = inverse(rank_map)

    outs = None
    up, down = {}, {}
    firsts = [sum(CHUNKS[:c]) * tile for c in range(len(CHUNKS))]

    def step(c, t):
        ups = [(i, i + 1) for i in range(t - 1, depth - 1)]
        downs = [(i, i - 1) for i in range(1, depth - t + 1)]
        down[c, t] = lax.ppermute(down[c, t - 1], "dp", downs)
        up[c, t] = lax.ppermute(up[c, t - 1], "dp", ups)

    def settle(outs, c, t):
        if t == 0:
            return place(outs, up[c, 0], level * rows + firsts[c], level >= 0, total, tile)
        outs = place(outs, down[c, t], (level + t) * rows + firsts[c], level + t < depth, total, tile)
        return place(outs, up[c, t], (level - t) * rows + firsts[c], level >= t, total, tile)

    for stage in range(len(CHUNKS) + depth - 1):
        if stage < len(CHUNKS):
            packed = pack(weight, inv, firsts[stage], CHUNKS[stage] * tile, tile)
            moved = lax.all_to_all(packed, "mp", split_axis=0, concat_axis=0, tiled=True)
            up[stage, 0] = down[stage, 0] = moved
        for t in range(1, depth):
            c = stage + 1 - t
            if 0 <= c < len(CHUNKS):
                step(c, t)
        for t in range(0, depth):
            c = stage - t
            if 0 <= c < len(CHUNKS):
                outs = settle(outs, c, t)

    divisor = 127.0 * math.sqrt(D * LANES)
    nblocks = cols // LANES
    partial_value = jnp.sum(column_sums(weight, tile).reshape(8, nblocks, LANES), axis=(0, 2))
    whole = jnp.zeros((nblocks * count,), jnp.float32)
    whole = lax.dynamic_update_slice_in_dim(whole, partial_value, rank * nblocks, 0)
    totals = lax.psum(whole, ("dp", "mp"))
    return (outs[0], outs[1], totals / divisor)


def solution(mesh):
    in_specs = (P("dp", "mp"), P())
    out_specs = (P(None, "mp"), P(None, "mp"), P())
    return jax.shard_map(local, mesh=mesh, in_specs=in_specs, out_specs=out_specs, check_vma=False)
```
